8 devices in a mesh: dp: 1 (over z), sp: 8 (over x, y, core).
Axes of the slice: x: 2, y: 2, z: 1, core: 2. Of those that a mesh axis runs over, the one named last changes fastest.
Arguments:
- x: bfloat16 [2048, 9216], P(('dp', 'sp'))
- gain: bfloat16 [9216], replicated
- wq: bfloat16 [9216, 9216], replicated
- wk: bfloat16 [9216, 9216], replicated
- wv: bfloat16 [9216, 9216], replicated
- wo: bfloat16 [9216, 9216], replicated
Outputs:
- output: bfloat16 [2048, 9216], P(('dp', 'sp'))
All inputs are finite; a program needn't handle non-finite values.
Results may differ from the reference program's by a relative error of at most 0.012.
Values are sent between devices in bfloat16 or wider.
A program may use at most 2 GiB of HBM per device.

```python
import jax
import jax.numpy as jnp
from jax import lax

ROWS = 2048
D = 9216
HEADS = 72
KV_HEADS = 72
HEAD = 128
THETA = 10000


def setup_inputs(seed: int = 0, part: int = 0) -> dict:
    kx, kn, kq, kk, kv, ko = jax.random.split(jax.random.key(seed), 6)

    def weights(key, rows, columns):
        return jax.random.normal(key, (rows, columns), jnp.float32) * rows**-0.5

    drawn = {
        "x": jax.random.normal(jax.random.fold_in(kx, part), (ROWS, D), jnp.float32),
        "gain": 1 + 0.1 * jax.random.normal(kn, (D,), jnp.float32),
        "wq": 2 * weights(kq, D, HEADS * HEAD),
        "wk": 2 * weights(kk, D, KV_HEADS * HEAD),
        "wv": 4 * weights(kv, D, KV_HEADS * HEAD),
        "wo": weights(ko, HEADS * HEAD, D),
    }
    return {k: v.astype(jnp.bfloat16) for k, v in drawn.items()}


def normed(x, gain):
    wide = x.astype(jnp.float32)
    scale = lax.rsqrt(jnp.mean(wide * wide, -1, keepdims=True) + 1e-6)
    return (wide * scale * gain.astype(jnp.float32)).astype(jnp.bfloat16)


def turned(t, place, theta):
    half = t.shape[-1] // 2
    angle = place.astype(jnp.float32)[:, None] * theta ** (-jnp.arange(half, dtype=jnp.float32) / half)
    cos, sin = jnp.cos(angle)[:, None], jnp.sin(angle)[:, None]
    a, b = t[..., :half].astype(jnp.float32), t[..., half:].astype(jnp.float32)
    return jnp.concatenate([a * cos - b * sin, b * cos + a * sin], -1).astype(jnp.bfloat16)


def matmul(a, w):
    return jnp.dot(a, w, preferred_element_type=jnp.float32).astype(jnp.bfloat16)


def einsum(form, a, b):
    return jnp.einsum(form, a.astype(jnp.float32), b.astype(jnp.float32))


def attention(q, k, v):
    scores = einsum("tgsd,ugd->gstu", q, k) * q.shape[-1] ** -0.5
    token = jnp.arange(q.shape[0])
    scores = jnp.where(token[:, None] >= token, scores, -jnp.inf)
    weights = jax.nn.softmax(scores, -1).astype(jnp.bfloat16)
    return einsum("gstu,ugd->tgsd", weights, v).astype(jnp.bfloat16)


def reference(x, gain, wq, wk, wv, wo):
    a, place = normed(x, gain), jnp.arange(ROWS)
    q = turned(matmul(a, wq).reshape(ROWS, HEADS, HEAD), place, THETA).reshape(ROWS, KV_HEADS, -1, HEAD)
    k = turned(matmul(a, wk).reshape(ROWS, KV_HEADS, HEAD), place, THETA)
    v = matmul(a, wv).reshape(ROWS, KV_HEADS, HEAD)
    seen = attention(q, k, v).reshape(ROWS, HEADS * HEAD)
    return (x.astype(jnp.float32) + jnp.dot(seen, wo, preferred_element_type=jnp.float32)).astype(jnp.bfloat16)
```

```python
import functools

import jax
import jax.numpy as jnp
from jax import lax
from jax.experimental import pallas as pl
from jax.experimental.pallas import tpu as pltpu
from jax.sharding import PartitionSpec as P

HEAD = 128
THETA = 10000
EPS = 1e-6
LOG2E = 1.4426950408889634
HIDDEN = -2e30
CHIPS, CORES = 4, 2
WBUF = 3
OBUF = 3
WOBUF = 4
BLOCK, PIECE = 256, 512
STRIP = 1536
BF16, F32 = jnp.bfloat16, jnp.float32


def _dot(a, b, ca, cb):
    return lax.dot_general(a, b, (((ca,), (cb,)), ((), ())), preferred_element_type=F32)


def _peer(chip, core):
    return {"sp": chip * CORES + core}


def _greet(peers):
    barrier = pltpu.get_barrier_semaphore()
    for peer in peers:
        pl.semaphore_signal(barrier, inc=1, device_id=peer, device_id_type=pl.DeviceIdType.MESH)
    pl.semaphore_wait(barrier, len(peers))


def _project(x_ref, gain_ref, cos_ref, sin_ref, wq_ref, wk_ref, wv_ref, out_ref, a_s, w_s, o_s, w_sem, pair_send, pair_recv, send_sem, recv_sem, own_sem):
    own, d = x_ref.shape
    rows = CORES * own
    tile = CHIPS * HEAD
    tiles = d // CORES // tile
    steps = 3 * tiles
    me = lax.axis_index("sp")
    chip, core = me // CORES, me % CORES
    weights = (wq_ref, wk_ref, wv_ref)

    def fetch(s, slot):
        j, t = s // 3, s % 3
        for n, w in enumerate(weights):
            @pl.when(t == n)
            def _():
                pltpu.make_async_copy(w.at[:, pl.ds(core * (d // CORES) + j * tile, tile)], w_s.at[slot], w_sem.at[slot]).start()

    for s in range(WBUF):
        fetch(s, s)

    step = 32
    mine = core * own

    def norm(i, _):
        here = pl.ds(i * step, step)
        wide = x_ref[here, :].astype(F32)
        scale = lax.rsqrt(jnp.mean(wide * wide, -1, keepdims=True) + EPS)
        a_s[pl.ds(mine + i * step, step), :] = (wide * scale * gain_ref[...]).astype(BF16)
        return _

    lax.fori_loop(0, own // step, norm, None)
    _greet([_peer(chip, 1 - core)] + [_peer(chip ^ r, core) for r in range(1, CHIPS)])
    pair = pltpu.make_async_remote_copy(
        src_ref=a_s.at[pl.ds(mine, own)], dst_ref=a_s.at[pl.ds(mine, own)], send_sem=pair_send, recv_sem=pair_recv,
        device_id=_peer(chip, 1 - core), device_id_type=pl.DeviceIdType.MESH)
    pair.start()

    def sends(s, slot):
        j, t = s // 3, s % 3
        there = out_ref.at[t, j, pl.ds(chip * rows, rows)]
        away = [
            pltpu.make_async_remote_copy(
                src_ref=o_s.at[slot, chip ^ r], dst_ref=there, send_sem=send_sem.at[slot, r], recv_sem=recv_sem.at[r],
                device_id=_peer(chip ^ r, core), device_id_type=pl.DeviceIdType.MESH)
            for r in range(1, CHIPS)
        ]
        return away, pltpu.make_async_copy(o_s.at[slot, chip], there, own_sem.at[slot])

    def sent(s):
        away, stays = sends(s, s % OBUF)
        for copy in away:
            copy.wait_send()
        stays.wait()

    def loaded(slot):
        pltpu.make_async_copy(wq_ref.at[:, pl.ds(0, tile)], w_s.at[slot], w_sem.at[slot]).wait()

    def make(s, slot, out, first, count):
        here = pl.ds(first, count)
        made = jnp.dot(a_s[here, :], w_s[slot], preferred_element_type=F32).astype(BF16)
        still = s % 3 == 2
        cos = jnp.where(still, 1.0, cos_ref[here, :])
        sin = jnp.where(still, 0.0, sin_ref[here, :])
        for i in range(CHIPS):
            t = made[:, i * HEAD : (i + 1) * HEAD].astype(F32)
            o_s[out, i, here, :] = (t * cos + pltpu.roll(t, HEAD // 2, axis=1) * sin).astype(BF16)

    def send(s, out):
        away, stays = sends(s, out)
        for copy in away:
            copy.start()
        stays.start()

    early = WBUF - 1

    def begin(s, _):
        loaded(s)
        make(s, s, s, mine, own)
        return _

    lax.fori_loop(0, early, begin, None)
    pair.wait()

    def complete(s, _):
        make(s, s, s, own - mine, own)
        fetch(s + WBUF, s)
        send(s, s)
        return _

    lax.fori_loop(0, early, complete, None)

    def one(s, _):
        @pl.when((s > early) & (s + WBUF - 1 < steps))
        def _():
            fetch(s + WBUF - 1, (s + WBUF - 1) % WBUF)

        loaded(s % WBUF)

        @pl.when(s >= OBUF)
        def _():
            sent(s - OBUF)

        make(s, s % WBUF, s % OBUF, 0, rows)
        send(s, s % OBUF)
        return _

    lax.fori_loop(early, steps, one, None)
    for s in range(steps - OBUF, steps):
        sent(s)
    for r in range(1, CHIPS):
        part = out_ref.at[:, :, pl.ds((chip ^ r) * rows, rows)]
        pltpu.make_async_remote_copy(
            src_ref=part, dst_ref=part, send_sem=send_sem.at[0, r], recv_sem=recv_sem.at[r],
            device_id=_peer(chip ^ r, core), device_id_type=pl.DeviceIdType.MESH).wait_recv()


def project(x, gain, cos, sin, wq, wk, wv):
    own, d = x.shape
    rows, tile = CORES * own, CHIPS * HEAD
    tiles = d // CORES // tile
    vmem, hbm = pl.BlockSpec(memory_space=pltpu.VMEM), pl.BlockSpec(memory_space=pltpu.HBM)
    return pl.pallas_call(
        _project,
        in_specs=[vmem] * 4 + [hbm] * 3,
        out_specs=hbm,
        out_shape=jax.ShapeDtypeStruct((3, tiles, CHIPS * rows, HEAD), BF16),
        scratch_shapes=[
            pltpu.VMEM((rows, d), BF16),
            pltpu.VMEM((WBUF, d, tile), BF16),
            pltpu.VMEM((OBUF, CHIPS, rows, HEAD), BF16),
            pltpu.SemaphoreType.DMA((WBUF,)),
            pltpu.SemaphoreType.DMA,
            pltpu.SemaphoreType.DMA,
            pltpu.SemaphoreType.DMA((OBUF, CHIPS)),
            pltpu.SemaphoreType.DMA((CHIPS,)),
            pltpu.SemaphoreType.DMA((OBUF,)),
        ],
        compiler_params=pltpu.CompilerParams(collective_id=0, has_side_effects=True, vmem_limit_bytes=62 * 2**20),
    )(x, gain, cos, sin, wq, wk, wv)


def _attend(qkv_ref, x_ref, wo_ref, out_ref, in_s, o_s, all_s, sum_s, w_s, y_s, in_sem, send_sem, recv_sem, w_sem, y_sem, *, block, piece):
    _, heads, tokens, _ = qkv_ref.shape
    own, d = out_ref.shape
    n = CHIPS * CORES
    me = lax.axis_index("sp")
    chip, core = me // CORES, me % CORES
    e = HEAD**-0.5 * LOG2E
    deep, wide = w_s.shape[1:]
    parts = d // wide
    steps = heads * CORES * parts

    def load(j, slot):
        return pltpu.make_async_copy(qkv_ref.at[:, j], in_s.at[slot], in_sem.at[slot])

    def fetch(s):
        j, k, part = s // (CORES * parts), s // parts % CORES, s % parts
        rows = pl.ds((k * heads + j) * deep, deep)
        return pltpu.make_async_copy(wo_ref.at[rows, pl.ds(part * wide, wide)], w_s.at[s % WOBUF], w_sem.at[s % WOBUF])

    load(0, 0).start()
    for s in range(WOBUF):
        fetch(s).start()
    sum_s[...] = x_ref[...].astype(F32)
    _greet([{"sp": me ^ r} for r in range(1, n)])

    def sends(j):
        return [
            pltpu.make_async_remote_copy(
                src_ref=o_s.at[j, me ^ r], dst_ref=all_s.at[j, core, chip], send_sem=send_sem.at[j, r], recv_sem=recv_sem.at[j, r],
                device_id={"sp": me ^ r}, device_id_type=pl.DeviceIdType.MESH)
            for r in range(1, n)
        ]

    ones = jnp.ones((8, tokens), BF16)
    order = lax.broadcasted_iota(jnp.int32, (block, block), 1) >= lax.broadcasted_iota(jnp.int32, (block, block), 0)

    def one(j, _):
        slot = j % 2

        @pl.when(j + 1 < heads)
        def _():
            load(j + 1, 1 - slot).start()

        load(j, slot).wait()

        values = jnp.concatenate([in_s[slot, 2].T, ones], axis=0)

        def score(b, c):
            keys, q = in_s[slot, 1, c * piece : min((c + 1) * piece, (b + 1) * block), :], in_s[slot, 0, b * block : (b + 1) * block, :]
            s = _dot(keys, q, 1, 1)
            if (c + 1) * piece < (b + 1) * block:
                return s
            whole = s.shape[0] - block
            last = jnp.where(order, s[whole:], HIDDEN)
            return jnp.concatenate([s[:whole], last], axis=0) if whole else last

        def pieces(b):
            return pl.cdiv((b + 1) * block, piece)

        blocks = tokens // block
        line = list(range(blocks - 1, -1, -1))
        scores = [score(line[0], c) for c in range(pieces(line[0]))]
        for at, b in enumerate(line):
            top = functools.reduce(jnp.maximum, [s.max(axis=0, keepdims=True) for s in scores])
            later, mix = [], None
            for c, s in enumerate(scores):
                if at + 1 < blocks and c < pieces(line[at + 1]):
                    later.append(score(line[at + 1], c))
                weights = jnp.exp2((s - top) * e).astype(BF16)
                part = _dot(values[:, c * piece : c * piece + s.shape[0]], weights, 1, 0)
                mix = part if mix is None else mix + part
            seen = (mix[:HEAD] / mix[HEAD : HEAD + 1]).T.astype(BF16)
            for i in range(block // own):
                o_s[j, b * (block // own) + i] = seen[i * own : (i + 1) * own]
            scores = later
        for copy in sends(j):
            copy.start()
        all_s[j, core, chip] = o_s[j, me]
        return _

    lax.fori_loop(0, heads, one, None)

    def add(s, _):
        j, k, part = s // (CORES * parts), s // parts % CORES, s % parts

        @pl.when(s % (CORES * parts) == 0)
        def _():
            for copy in sends(j):
                copy.wait_recv()

        fetch(s).wait()
        seen = jnp.concatenate([all_s[j, k, c] for c in range(CHIPS)], axis=1)
        for i in range(0, wide, STRIP):
            here = pl.ds(pl.multiple_of(part * wide + i, STRIP), STRIP)
            sum_s[:, here] += jnp.dot(seen, w_s[s % WOBUF, :, i : i + STRIP], preferred_element_type=F32)

        @pl.when(s + WOBUF < steps)
        def _():
            fetch(s + WOBUF).start()

        return _

    lax.fori_loop(0, steps - parts, add, None)
    outs = []
    for part in range(parts):
        add(steps - parts + part, None)
        here = pl.ds(part * wide, wide)
        y_s[:, here] = sum_s[:, here].astype(BF16)
        outs.append(pltpu.make_async_copy(y_s.at[:, here], out_ref.at[:, here], y_sem.at[part]))
        outs[-1].start()
    for copy in outs:
        copy.wait()

    def sent(j, _):
        for copy in sends(j):
            copy.wait_send()
        return _

    lax.fori_loop(0, heads, sent, None)


def attend(qkv, x, wo):
    _, heads, tokens, _ = qkv.shape
    own, d = x.shape
    n = CHIPS * CORES
    hbm, vmem = pl.BlockSpec(memory_space=pltpu.HBM), pl.BlockSpec(memory_space=pltpu.VMEM)
    return pl.pallas_call(
        functools.partial(_attend, block=BLOCK, piece=PIECE),
        in_specs=[hbm, vmem, hbm],
        out_specs=hbm,
        out_shape=jax.ShapeDtypeStruct((own, d), BF16),
        scratch_shapes=[
            pltpu.VMEM((2, 3, tokens, HEAD), BF16),
            pltpu.VMEM((heads, n, own, HEAD), BF16),
            pltpu.VMEM((heads, CORES, CHIPS, own, HEAD), BF16),
            pltpu.VMEM((own, d), F32),
            pltpu.VMEM((WOBUF, CHIPS * HEAD, d // 2), BF16),
            pltpu.VMEM((own, d), BF16),
            pltpu.SemaphoreType.DMA((2,)),
            pltpu.SemaphoreType.DMA((heads, n)),
            pltpu.SemaphoreType.DMA((heads, n)),
            pltpu.SemaphoreType.DMA((WOBUF,)),
            pltpu.SemaphoreType.DMA((2,)),
        ],
        compiler_params=pltpu.CompilerParams(collective_id=1, has_side_effects=True, vmem_limit_bytes=62 * 2**20),
    )(qkv, x, wo)


def solution(mesh):
    def step(x, gain, wq, wk, wv, wo):
        own = x.shape[0]
        chip = lax.axis_index("sp") // CORES
        half = HEAD // 2
        place = chip * CORES * own + jnp.arange(CORES * own)
        angle = place.astype(F32)[:, None] * THETA ** (-jnp.arange(half, dtype=F32) / half)
        cos, sin = jnp.cos(angle), jnp.sin(angle)
        qkv = project(x, gain.astype(F32)[None], jnp.concatenate([cos, cos], -1), jnp.concatenate([-sin, sin], -1), wq, wk, wv)
        return attend(qkv, x, wo)

    tokens, whole = P(("dp", "sp"), None), P(None, None)
    return jax.shard_map(
        step,
        mesh=mesh,
        in_specs=(tokens, P(None), whole, whole, whole, whole),
        out_specs=tokens,
        check_vma=False,
    )
```
